1024 devices in a mesh: gx: 16 (over x_hi, y, core), gy: 64 (over z, x_lo).
Axes of the slice: x: 4 (x_hi: 2, x_lo: 2; x = x_hi * 2 + x_lo), y: 4, z: 32, core: 2. Of those that a mesh axis runs over, the one named last changes fastest.
Arguments:
- conserved: float32 [5, 64, 1024, 128], P(None, 'gx', 'gy'), as said below
Outputs:
- increment: float32 [5, 64, 1024, 128], P(None, 'gx', 'gy')
- blending: float32 [16, 256, 32], P('gx', 'gy')
Inputs may be any that keep to these rules, and one draw needn't show every extreme that they name: `conserved`: every node's density and pressure are positive.
All inputs are finite; a program needn't handle non-finite values. Where the reference program divides by a largest or mean magnitude, that divisor is 1e-20 or more.
Results may differ from the reference program's by a relative error of at most 0.0003.
Values sent between devices are 32-bit elements; how exact they have to be, the bound alone decides.
No kernel may reach another device: no remote copies, remote signals or barrier semaphores. Data moves between devices by JAX's collectives and lax.ppermute only.
A program may use at most 32 MiB of HBM per device.

```python
import math
import jax
import jax.numpy as jnp
import numpy as np
from jax import lax

EZ = 32
EX = 16
EY = 256


def log_uniform(subkey, lower, upper, layout):
    return jnp.exp(jax.random.uniform(subkey, layout, jnp.float32, math.log(lower), math.log(upper)))


def draw_conserved(key, part):
    subkeys = jax.random.split(key, 7)
    element_shape = (EX, 1, EY, 1, EZ, 1)
    node_shape = (EX, 4, EY, 4, EZ, 4)
    inverse_root = 1.0 / math.sqrt(5.0)
    points = jnp.array([-1.0, -inverse_root, inverse_root, 1.0], jnp.float32)
    coord_x = points.reshape(1, 4, 1, 1, 1, 1)
    coord_y = points.reshape(1, 1, 1, 4, 1, 1)
    coord_z = points.reshape(1, 1, 1, 1, 1, 4)
    index_x = jnp.arange(EX, dtype=jnp.int32).reshape(EX, 1, 1, 1, 1, 1)
    index_y = jnp.arange(EY, dtype=jnp.int32).reshape(1, 1, EY, 1, 1, 1)
    index_z = jnp.arange(EZ, dtype=jnp.int32).reshape(1, 1, 1, 1, EZ, 1)
    rough = (2 * index_x + index_y + 3 * index_z) % 8 == 0
    amplitude = jnp.where(rough, log_uniform(subkeys[0], 0.1, 0.2, element_shape), 0.0)
    base_density = log_uniform(subkeys[1], 0.5, 2.0, element_shape)
    base_pressure = log_uniform(subkeys[2], 0.5, 2.0, element_shape)
    base_velocity = 0.3 * jax.random.normal(subkeys[3], (3,) + element_shape, jnp.float32)
    density_slopes = jax.random.uniform(subkeys[5], (3,) + element_shape, jnp.float32, -1.0, 1.0)
    velocity_slopes = jax.random.uniform(subkeys[6], (3, 3) + element_shape, jnp.float32, -1.0, 1.0)
    jitter = jnp.clip(jax.random.normal(subkeys[4], (5,) + node_shape, jnp.float32), -4.0, 4.0)
    linear_density = 1.0 + 0.3 * (density_slopes[0] * coord_x + density_slopes[1] * coord_y + density_slopes[2] * coord_z)
    linear_velocity = 0.6 * (velocity_slopes[:, 0] * coord_x + velocity_slopes[:, 1] * coord_y + velocity_slopes[:, 2] * coord_z)
    layout = (4 * EX, 4 * EY, 4 * EZ)
    density = (base_density * linear_density * jnp.exp(amplitude * jitter[0])).reshape(layout)
    pressure = jnp.broadcast_to(base_pressure * jnp.exp(amplitude * jitter[1]), node_shape).reshape(layout)
    velocity = (base_velocity + linear_velocity + amplitude * jitter[2:5]).reshape((3,) + layout)
    energy = pressure / 0.4 + 0.5 * density * jnp.sum(velocity * velocity, axis=0)
    return jnp.stack([density, density * velocity[0], density * velocity[1], density * velocity[2], energy]).astype(jnp.float32)


def setup_inputs(seed: int = 0) -> dict:
    key_of = jax.random.split(jax.random.key(seed), 2)
    return {
        "conserved": draw_conserved(jax.random.fold_in(key_of[1], 71), 0),
    }


gas_gamma = 1.4

def tables():
    inverse_root = 1.0 / math.sqrt(5.0)
    points = np.array([-1.0, -inverse_root, inverse_root, 1.0])
    weights = [1.0 / 6.0, 5.0 / 6.0, 5.0 / 6.0, 1.0 / 6.0]
    barycentric = np.array([1.0 / np.prod([points[target] - points[other] for other in range(4) if other != target]) for target in range(4)])
    derivative = np.zeros((4, 4))
    for target in range(4):
        for source in range(4):
            if target != source:
                derivative[target, source] = barycentric[source] / barycentric[target] / (points[target] - points[source])
    legendre = np.stack([np.ones(4), points, (3.0 * points ** 2 - 1.0) / 2.0, (5.0 * points ** 3 - 3.0 * points) / 2.0], 1)
    legendre = legendre * np.sqrt(np.arange(4) + 0.5)
    weight_column = np.array(weights)[:, None]
    discrete_norms = np.sum(weight_column * legendre * legendre, 0)
    inverse = (weight_column * legendre).T / discrete_norms[:, None]
    return (weights, derivative, inverse)

def describe(conserved):
    density = conserved[0]
    velocity = conserved[1:4] / density
    pressure = (gas_gamma - 1.0) * (conserved[4] - 0.5 * density * lax.optimization_barrier(jnp.sum(velocity * velocity, axis=0)))
    sound_speed = jnp.sqrt(gas_gamma * pressure / density)
    return (conserved, density, velocity, pressure, sound_speed)

def log_mean(left_value, right_value):
    relative = (left_value - right_value) / (left_value + right_value)
    square = relative * relative
    series = 1.0 + square / 3.0 + square * square / 5.0 + square * square * square / 7.0
    safe_relative = jnp.where(square < 0.01, 1.0, relative)
    logarithmic = jnp.log(left_value / right_value) / (2.0 * safe_relative)
    factor = jnp.where(square < 0.01, series, logarithmic)
    return (left_value + right_value) / (2.0 * factor)

def entropy_flux(left_state, right_state, normal):
    left_density, left_velocity, left_pressure = (left_state[1], left_state[2], left_state[3])
    right_density, right_velocity, right_pressure = (right_state[1], right_state[2], right_state[3])
    mean_density = log_mean(left_density, right_density)
    inverse_beta = 1.0 / log_mean(left_density / left_pressure, right_density / right_pressure)
    mean_velocity = 0.5 * (left_velocity + right_velocity)
    mean_pressure = 0.5 * (left_pressure + right_pressure)
    square_mean = 0.5 * lax.optimization_barrier(jnp.sum(left_velocity * right_velocity, axis=0))
    mass_flux = mean_density * mean_velocity[normal]
    components = [mass_flux]
    for other in range(3):
        momentum = mass_flux * mean_velocity[other]
        if other == normal:
            momentum = momentum + mean_pressure
        components.append(momentum)
    energy_flux = mass_flux * (square_mean + inverse_beta / (gas_gamma - 1.0)) + 0.5 * (left_pressure * right_velocity[normal] + right_pressure * left_velocity[normal])
    components.append(energy_flux)
    return jnp.stack(components)

def surface_flux(left_state, right_state, normal):
    largest = jnp.maximum(jnp.abs(left_state[2][normal]) + left_state[4], jnp.abs(right_state[2][normal]) + right_state[4])
    return entropy_flux(left_state, right_state, normal) - 0.5 * largest * (right_state[0] - left_state[0])

def accumulate(total, term):
    return term if total is None else total + term

def direction_terms(padded, dimension):
    weights, derivative, inverse = tables()
    elements = (padded.shape[dimension] - 2) // 4

    def nodes_from(start):
        return describe(lax.slice_in_dim(padded, start, start + 4 * (elements - 1) + 1, 4, dimension))
    node_states = [nodes_from(1 + position) for position in range(4)]
    previous = nodes_from(0)
    following = nodes_from(5)
    normal = dimension - 1
    high_order = [None, None, None, None]
    for first in range(4):
        for second in range(first + 1, 4):
            pair_flux = entropy_flux(node_states[first], node_states[second], normal)
            high_order[first] = accumulate(high_order[first], 2.0 * float(derivative[first, second]) * pair_flux)
            high_order[second] = accumulate(high_order[second], 2.0 * float(derivative[second, first]) * pair_flux)
    lower_face = surface_flux(previous, node_states[0], normal)
    upper_face = surface_flux(node_states[3], following, normal)
    high_order[0] = high_order[0] - lower_face / weights[0]
    high_order[3] = high_order[3] + upper_face / weights[3]
    face_flux = [lower_face] + [surface_flux(node_states[position], node_states[position + 1], normal) for position in range(3)] + [upper_face]
    subcell = [(face_flux[position + 1] - face_flux[position]) / weights[position] for position in range(4)]
    layout = list(padded.shape)
    layout[dimension] = 4 * elements
    return (jnp.stack(high_order, dimension + 1).reshape(layout), jnp.stack(subcell, dimension + 1).reshape(layout))

def tendency(padded, blend_weights):
    along_x = padded[:, :, 1:-1]
    along_y = padded[:, 1:-1]
    center = padded[:, 1:-1, 1:-1]
    along_z = jnp.concatenate([center[..., -1:], center, center[..., :1]], axis=3)
    high_x, subcell_x = direction_terms(along_x, 1)
    high_y, subcell_y = direction_terms(along_y, 2)
    high_z, subcell_z = direction_terms(along_z, 3)
    high_total = high_x + high_y + high_z
    subcell_total = subcell_x + subcell_y + subcell_z
    return -((1.0 - blend_weights) * high_total + blend_weights * subcell_total)

def indicator(conserved):
    weights, derivative, inverse = tables()
    state = describe(conserved)
    indicated = state[1] * state[3]
    extent = indicated.shape
    grouped = indicated.reshape(extent[0] // 4, 4, extent[1] // 4, 4, extent[2] // 4, 4)
    matrix = jnp.asarray(inverse, jnp.float32)
    coefficients = jnp.einsum('ai,bj,ck,xiyjzk->abcxyz', matrix, matrix, matrix, grouped, precision=lax.Precision.HIGHEST)
    squares = coefficients * coefficients
    energy_all = lax.optimization_barrier(jnp.sum(squares, axis=(0, 1, 2)))
    energy_three = lax.optimization_barrier(jnp.sum(squares[:3, :3, :3], axis=(0, 1, 2)))
    energy_two = lax.optimization_barrier(jnp.sum(squares[:2, :2, :2], axis=(0, 1, 2)))
    energy = jnp.maximum((energy_all - energy_three) / (energy_all + 1e-06), (energy_three - energy_two) / (energy_three + 1e-06))
    threshold = 0.5 * 10.0 ** (-1.8 * 4.0 ** 0.25)
    sharpness = math.log(9999.0)
    raw_blend = 1.0 / (1.0 + jnp.exp(-(sharpness / threshold) * (energy - threshold)))
    return jnp.minimum(raw_blend, 0.5)

def smooth(raw_blend, x_lower, x_upper, y_lower, y_upper):
    extended_x = jnp.concatenate([x_lower, raw_blend, x_upper], axis=0)
    extended_y = jnp.concatenate([y_lower, raw_blend, y_upper], axis=1)
    neighbours = jnp.maximum(extended_x[:-2], extended_x[2:])
    neighbours = jnp.maximum(neighbours, jnp.maximum(extended_y[:, :-2], extended_y[:, 2:]))
    neighbours = jnp.maximum(neighbours, jnp.maximum(jnp.roll(raw_blend, 1, 2), jnp.roll(raw_blend, -1, 2)))
    return jnp.maximum(raw_blend, 0.5 * neighbours)

def blend_nodes(blending):
    extent = blending.shape
    spread = jnp.broadcast_to(blending[:, None, :, None, :, None], (extent[0], 4, extent[1], 4, extent[2], 4))
    return spread.reshape(4 * extent[0], 4 * extent[1], 4 * extent[2])

def reference(conserved):
    state = describe(conserved)
    top_speed = jnp.max(lax.optimization_barrier(jnp.sum(jnp.abs(state[2]), axis=0)) + 3.0 * state[4])
    time_step = 0.25 / top_speed
    raw_blend = indicator(conserved)
    blending = smooth(raw_blend, raw_blend[-1:], raw_blend[:1], raw_blend[:, -1:], raw_blend[:, :1])
    blend_full = blend_nodes(blending)
    nodes_x = conserved.shape[1]

    def column(column_index):
        positions = (4 * column_index - 1 + jnp.arange(6, dtype=jnp.int32)) % nodes_x
        slab_state = jnp.take(conserved, positions.astype(jnp.int32), axis=1)
        slab_state = jnp.concatenate([slab_state[:, :, -1:], slab_state, slab_state[:, :, :1]], axis=2)
        slab_blend = lax.dynamic_slice_in_dim(blend_full, (4 * column_index).astype(jnp.int32), 4, 0)
        return time_step * tendency(slab_state, slab_blend)
    columns = lax.map(column, jnp.arange(nodes_x // 4, dtype=jnp.int32))
    increment = jnp.transpose(columns, (1, 0, 2, 3, 4)).reshape(conserved.shape)
    return (increment, blending)
```

```python
import functools
import math

import jax
import jax.numpy as jnp
import numpy as np
from jax import lax
from jax.experimental import pallas as pl
from jax.experimental.pallas import tpu as pltpu
from jax.sharding import Mesh
from jax.sharding import PartitionSpec as P

GX = ("gx_0", "gx_1", "gx_2")
GY = ("gy_0", "gy_1")
EVERY = GX + GY
SIZES = (2, 4, 2, 32, 2)

VMEM_BYTES = 6 << 20

WEIGHTS = (1.0 / 6.0, 5.0 / 6.0, 5.0 / 6.0, 1.0 / 6.0)


def tables():
    inverse_root = 1.0 / math.sqrt(5.0)
    points = np.array([-1.0, -inverse_root, inverse_root, 1.0])
    barycentric = np.array(
        [
            1.0 / np.prod([points[target] - points[other] for other in range(4) if other != target])
            for target in range(4)
        ]
    )
    derivative = np.zeros((4, 4))
    for target in range(4):
        for source in range(4):
            if target != source:
                derivative[target, source] = (
                    barycentric[source] / barycentric[target] / (points[target] - points[source])
                )
    legendre = np.stack(
        [np.ones(4), points, (3.0 * points**2 - 1.0) / 2.0, (5.0 * points**3 - 3.0 * points) / 2.0],
        1,
    )
    legendre = legendre * np.sqrt(np.arange(4) + 0.5)
    weight_column = np.array(WEIGHTS)[:, None]
    discrete_norms = np.sum(weight_column * legendre * legendre, 0)
    inverse = (weight_column * legendre).T / discrete_norms[:, None]
    return derivative, inverse


DERIVATIVE, INVERSE = tables()
SPLIT = [[2.0 * WEIGHTS[k] * float(DERIVATIVE[k, j]) for j in range(4)] for k in range(4)]


def roll(value, shift, axis):
    size = value.shape[axis]
    return pltpu.roll(value, shift % size, axis)


def local_node(shape, axis):
    return lax.broadcasted_iota(jnp.int32, shape, axis) % 4


def by_node(node, values):
    out = jnp.full(node.shape, values[3], jnp.float32)
    for k in range(3):
        out = jnp.where(node == k, jnp.float32(values[k]), out)
    return out


def primitives(parts):
    density = parts[0]
    inverse = 1.0 / density
    velocity = [parts[1 + d] * inverse for d in range(3)]
    square = velocity[0] * velocity[0] + velocity[1] * velocity[1] + velocity[2] * velocity[2]
    pressure = 0.4 * (parts[4] - 0.5 * density * square)
    return density, velocity, pressure, inverse


def sound_of(pressure, inverse):
    return jnp.sqrt(1.4 * pressure * inverse)


NAMES = ("r", "u", "v", "w", "p", "c", "s", "lr", "ls", "m1", "m2", "m3", "e")


def full_state(parts):
    density, velocity, pressure, inverse = primitives(parts)
    ratio = density / pressure
    return {
        "r": density,
        "u": velocity[0],
        "v": velocity[1],
        "w": velocity[2],
        "p": pressure,
        "c": sound_of(pressure, inverse),
        "s": ratio,
        "lr": jnp.log(density),
        "ls": jnp.log(ratio),
        "m1": parts[1],
        "m2": parts[2],
        "m3": parts[3],
        "e": parts[4],
    }


def mean_parts(a, b, log_a, log_b):
    total = a + b
    gap = a - b
    relative = gap / total
    square = relative * relative
    small = square < 0.01
    series = 1.0 + square * (1.0 / 3.0 + square * (1.0 / 5.0 + square * (1.0 / 7.0)))
    top = jnp.where(small, 0.5 * total, gap)
    bottom = jnp.where(small, series, log_a - log_b)
    return top, bottom


def pair_flux(a, b, normal):
    top, bottom = mean_parts(a["r"], b["r"], a["lr"], b["lr"])
    mass = top / bottom
    top, bottom = mean_parts(a["s"], b["s"], a["ls"], b["ls"])
    inverse_beta = bottom / top
    key = "uvw"[normal]
    flux0 = mass * (0.5 * (a[key] + b[key]))
    out = [flux0]
    for other in range(3):
        name = "uvw"[other]
        term = flux0 * (0.5 * (a[name] + b[name]))
        if other == normal:
            term = term + 0.5 * (a["p"] + b["p"])
        out.append(term)
    dot = 0.5 * (a["u"] * b["u"] + a["v"] * b["v"] + a["w"] * b["w"])
    out.append(
        flux0 * (dot + 2.5 * inverse_beta) + 0.5 * (a["p"] * b[key] + b["p"] * a[key])
    )
    return out


def dissipation(a, b, normal):
    key = "uvw"[normal]
    half = 0.5 * jnp.maximum(jnp.abs(a[key]) + a["c"], jnp.abs(b[key]) + b["c"])
    return [half * (b[q] - a[q]) for q in ("r", "m1", "m2", "m3", "e")]


def speed_kernel(conserved_ref, out_ref):
    best = None
    for x in range(4):
        density, velocity, pressure, inverse = primitives([conserved_ref[q, x] for q in range(5)])
        speed = (
            jnp.abs(velocity[0])
            + jnp.abs(velocity[1])
            + jnp.abs(velocity[2])
            + 3.0 * sound_of(pressure, inverse)
        )
        best = speed if best is None else jnp.maximum(best, speed)
    row = jnp.max(best, axis=0, keepdims=True)
    out_ref[...] = jnp.broadcast_to(row[None], out_ref.shape)


def forward_kernel(in_ref, out_ref):
    row = jnp.max(in_ref[...], axis=0, keepdims=True)
    out_ref[...] = jnp.broadcast_to(row, out_ref.shape)


def transform(value, axis):
    node = local_node(value.shape, axis)
    total = None
    for offset in range(-3, 4):
        coefficients = [
            float(INVERSE[a, a + offset]) if 0 <= a + offset < 4 else 0.0 for a in range(4)
        ]
        shifted = value if offset == 0 else roll(value, -offset, axis)
        term = by_node(node, coefficients) * shifted
        total = term if total is None else total + term
    return total


def spread_sum(value, axis):
    index = lax.broadcasted_iota(jnp.int32, value.shape, axis)
    for step in (1, 2):
        other = jnp.where((index // step) % 2 == 1, roll(value, step, axis), roll(value, -step, axis))
        value = value + other
    return value


def raw_blending(layers):
    indicated = []
    for parts in layers:
        density, _, pressure, _ = primitives(parts)
        indicated.append(density * pressure)
    shape = indicated[0].shape
    node_y, node_z = local_node(shape, 0), local_node(shape, 1)
    degree = jnp.maximum(node_y, node_z)
    high = mid = low = None
    zero = jnp.zeros(shape, jnp.float32)
    for a in range(4):
        modes = sum(float(INVERSE[a, k]) * indicated[k] for k in range(4))
        modes = transform(transform(modes, 0), 1)
        square = modes * modes
        if a == 3:
            high = high + square
            continue
        top = jnp.where(degree == 3, square, zero)
        high = top if high is None else high + top
        if a == 2:
            mid = mid + jnp.where(degree < 3, square, zero)
            continue
        middle = jnp.where(degree == 2, square, zero)
        mid = middle if mid is None else mid + middle
        rest = jnp.where(degree < 2, square, zero)
        low = rest if low is None else low + rest
    high, mid, low = (spread_sum(spread_sum(v, 0), 1) for v in (high, mid, low))
    three = low + mid
    energy = jnp.maximum(high / (three + high + 1e-06), mid / (three + 1e-06))
    threshold = 0.5 * 10.0 ** (-1.8 * 4.0**0.25)
    sharpness = math.log(9999.0)
    raw = 1.0 / (1.0 + jnp.exp(-(sharpness / threshold) * (energy - threshold)))
    return jnp.minimum(raw, 0.5)


def layers_kernel(conserved_ref, _, raw_ref, xlo_ref, xhi_ref, ylo_ref, yhi_ref):
    raw = raw_blending([[conserved_ref[q, x] for q in range(5)] for x in range(4)])
    raw_ref[...] = raw
    for q in range(5):
        xlo_ref[q] = conserved_ref[q, 0]
        xhi_ref[q] = conserved_ref[q, 3]
        for x in range(4):
            ylo_ref[q, x : x + 1] = conserved_ref[q, x, 0:1]
            yhi_ref[q, x : x + 1] = conserved_ref[q, x, 15:16]
    xlo_ref[5] = raw
    xhi_ref[5] = raw
    ylo_ref[5] = jnp.broadcast_to(raw[0:1], (4, 128))
    yhi_ref[5] = jnp.broadcast_to(raw[15:16], (4, 128))


def physics_kernel(
    conserved_ref, raw_ref, xprev_ref, xnext_ref, yprev_ref, ynext_ref, out_ref, blend_ref, state_ref
):
    raw = raw_ref[...]
    shape = raw.shape
    row = lax.broadcasted_iota(jnp.int32, shape, 0)
    node_y, node_z = row % 4, local_node(shape, 1)

    before = jnp.where(row < 4, jnp.broadcast_to(yprev_ref[5, 0:1], shape), roll(raw, 4, 0))
    after = jnp.where(row >= 12, jnp.broadcast_to(ynext_ref[5, 0:1], shape), roll(raw, -4, 0))
    around = jnp.maximum(xprev_ref[5], xnext_ref[5])
    around = jnp.maximum(around, jnp.maximum(before, after))
    around = jnp.maximum(around, jnp.maximum(roll(raw, 4, 1), roll(raw, -4, 1)))
    blend = jnp.maximum(raw, 0.5 * around)
    pick_z = (
        lax.broadcasted_iota(jnp.int32, (128, 32), 0) == 4 * lax.broadcasted_iota(jnp.int32, (128, 32), 1)
    ).astype(jnp.float32)
    compact = jnp.dot(
        blend, pick_z, precision=lax.Precision.HIGHEST, preferred_element_type=jnp.float32
    )
    for element in range(4):
        blend_ref[0, element : element + 1] = compact[4 * element : 4 * element + 1]
    keep = 1.0 - blend

    for x in range(4):
        state = full_state([conserved_ref[q, x] for q in range(5)])
        for i, name in enumerate(NAMES[:9]):
            state_ref[i, x] = state[name]

    def load(x):
        state = {name: state_ref[i, x] for i, name in enumerate(NAMES[:9])}
        for i, name in enumerate(NAMES[9:]):
            state[name] = conserved_ref[1 + i, x]
        return state

    def store(x, values, first=False):
        for q in range(5):
            out_ref[q, x] = values[q] if first else out_ref[q, x] + values[q]

    y_prev = full_state([yprev_ref[q] for q in range(5)])
    y_next = full_state([ynext_ref[q] for q in range(5)])
    edge = {}
    for i, name in enumerate(NAMES[:9]):
        edge[name] = jnp.concatenate([state_ref[i, x, 0:1] for x in range(4)], axis=0)
    for i, name in enumerate(NAMES[9:]):
        edge[name] = jnp.concatenate([conserved_ref[1 + i, x, 0:1] for x in range(4)], axis=0)
    low_face = [
        f - d for f, d in zip(pair_flux(y_prev, edge, 1), dissipation(y_prev, edge, 1), strict=True)
    ]

    def along(axis, node, x, state):
        normal = axis + 1
        one = jnp.ones(shape, jnp.float32)
        step = [SPLIT[0][1], SPLIT[1][2], SPLIT[2][3], 0.0]
        inner = node < 3
        weight_f = jnp.where(inner, keep * by_node(node, step) + blend, one)
        weight_d = jnp.where(inner, blend, one)
        weight_far = keep * by_node(node, [SPLIT[0][2], SPLIT[1][3], 0.0, SPLIT[3][0]])
        next_ = {}
        for name in NAMES:
            moved = roll(state[name], -1, axis)
            if axis == 0:
                moved = jnp.where(row == 15, jnp.broadcast_to(y_next[name][x : x + 1], shape), moved)
            next_[name] = moved
        flux = pair_flux(state, next_, normal)
        loss = dissipation(state, next_, normal)
        far = {
            name: jnp.where(node == 3, roll(state[name], 3, axis), roll(state[name], -2, axis))
            for name in ("r", "u", "v", "w", "p", "s", "lr", "ls")
        }
        cross = pair_flux(state, far, normal)
        inverse_weight = by_node(node, [-1.0 / w for w in WEIGHTS])
        out = []
        for q in range(5):
            near = weight_f * flux[q] - weight_d * loss[q]
            back = roll(near, 1, axis)
            if axis == 0:
                back = jnp.where(row == 0, jnp.broadcast_to(low_face[q][x : x + 1], shape), back)
            wide = weight_far * cross[q]
            taken = jnp.where(node >= 2, roll(wide, 2, axis), jnp.where(node == 0, roll(wide, -3, axis), 0.0))
            out.append(inverse_weight * (near - back + wide - taken))
        return out

    for x in range(4):
        state = load(x)
        in_y = along(0, node_y, x, state)
        in_z = along(1, node_z, x, state)
        store(x, [a + b for a, b in zip(in_y, in_z, strict=True)], first=True)

    def gather(other):
        return full_state([other[q] for q in range(5)])

    for first in range(4):
        for second in range(first + 1, 4):
            a, b = load(first), load(second)
            flux = pair_flux(a, b, 0)
            if second == first + 1:
                weight = keep * SPLIT[first][second] + blend
                loss = dissipation(a, b, 0)
                term = [weight * f - blend * d for f, d in zip(flux, loss, strict=True)]
            else:
                weight = keep * SPLIT[first][second]
                term = [weight * f for f in flux]
            store(first, [(-1.0 / WEIGHTS[first]) * t for t in term])
            store(second, [(1.0 / WEIGHTS[second]) * t for t in term])
    a, b = gather(xprev_ref), load(0)
    flux, loss = pair_flux(a, b, 0), dissipation(a, b, 0)
    store(0, [(1.0 / WEIGHTS[0]) * (f - d) for f, d in zip(flux, loss, strict=True)])
    a, b = load(3), gather(xnext_ref)
    flux, loss = pair_flux(a, b, 0), dissipation(a, b, 0)
    store(3, [(-1.0 / WEIGHTS[3]) * (f - d) for f, d in zip(flux, loss, strict=True)])


def scale_kernel(tendency_ref, speed_ref, out_ref):
    row = jnp.max(speed_ref[...], axis=0)
    top = jnp.max(row, axis=1, keepdims=True)
    step = 0.25 / top
    for q in range(5):
        for x in range(4):
            out_ref[q, x] = tendency_ref[q, x] * step


def call(kernel, outs, *args, scratch=(), **kwargs):
    return pl.pallas_call(
        kernel,
        out_shape=[jax.ShapeDtypeStruct(shape, jnp.float32) for shape in outs],
        scratch_shapes=list(scratch),
        compiler_params=pltpu.CompilerParams(vmem_limit_bytes=VMEM_BYTES),
        **kwargs,
    )(*args)


def shift(block, axes, step):
    count = math.prod(lax.axis_size(a) for a in axes)
    return lax.ppermute(block, axes, [(i, (i + step) % count) for i in range(count)])


def z_groups():
    order = [19] + [z for z in range(32) if z != 19]
    index = np.arange(1024).reshape(SIZES).transpose(0, 1, 2, 4, 3)[..., order]
    return index.reshape(-1, 32).tolist()


def plane_groups():
    index = np.arange(1024).reshape(SIZES).transpose(3, 0, 1, 2, 4).reshape(32, 32)
    lead = int(np.ravel_multi_index((1, 2, 1, 0), (2, 4, 2, 2)))
    order = [lead] + [i for i in range(32) if i != lead]
    return index[:, order].tolist()


def exchange(rows, groups):
    return lax.all_to_all(rows, EVERY, 0, 0, axis_index_groups=groups)


def body(conserved):
    (rows,) = call(speed_kernel, [(32, 1, 128)], conserved)
    column = exchange(rows, z_groups())
    raw, xlo, xhi, ylo, yhi = call(
        layers_kernel,
        [(16, 128), (6, 16, 128), (6, 16, 128), (6, 4, 128), (6, 4, 128)],
        conserved,
        rows,
    )
    xprev = shift(xhi, GX, 1)
    xnext = shift(xlo, GX, -1)
    yprev = shift(yhi, GY, 1)
    ynext = shift(ylo, GY, -1)
    (forward,) = call(forward_kernel, [(32, 1, 128)], column)
    speeds = exchange(forward, plane_groups())
    tendency, blending = call(
        physics_kernel,
        [(5, 4, 16, 128), (1, 4, 32)],
        conserved,
        raw,
        xprev,
        xnext,
        yprev,
        ynext,
        scratch=[pltpu.VMEM((9, 4, 16, 128), jnp.float32)],
    )
    (increment,) = call(scale_kernel, [(5, 4, 16, 128)], tendency, speeds)
    return increment, blending


def solution(mesh):
    split = Mesh(mesh.devices.reshape(SIZES), EVERY)
    return jax.shard_map(
        body,
        mesh=split,
        in_specs=(P(None, GX, GY, None),),
        out_specs=(P(None, GX, GY, None), P(GX, GY, None)),
        check_vma=False,
    )
```

```python
import math

import jax
import jax.numpy as jnp
import numpy as np
from jax import lax
from jax.experimental import pallas as pl
from jax.experimental.pallas import tpu as pltpu
from jax.sharding import Mesh
from jax.sharding import PartitionSpec as P


EVERY = ("gx", "gy")
SIZES = (2, 4, 2, 32, 2)

VMEM_BYTES = 6 << 20

WEIGHTS = (1.0 / 6.0, 5.0 / 6.0, 5.0 / 6.0, 1.0 / 6.0)


def tables():
    inverse_root = 1.0 / math.sqrt(5.0)
    points = np.array([-1.0, -inverse_root, inverse_root, 1.0])
    barycentric = np.array(
        [
            1.0 / np.prod([points[target] - points[other] for other in range(4) if other != target])
            for target in range(4)
        ]
    )
    derivative = np.zeros((4, 4))
    for target in range(4):
        for source in range(4):
            if target != source:
                derivative[target, source] = (
                    barycentric[source] / barycentric[target] / (points[target] - points[source])
                )
    legendre = np.stack(
        [np.ones(4), points, (3.0 * points**2 - 1.0) / 2.0, (5.0 * points**3 - 3.0 * points) / 2.0],
        1,
    )
    legendre = legendre * np.sqrt(np.arange(4) + 0.5)
    weight_column = np.array(WEIGHTS)[:, None]
    discrete_norms = np.sum(weight_column * legendre * legendre, 0)
    inverse = (weight_column * legendre).T / discrete_norms[:, None]
    return derivative, inverse


DERIVATIVE, INVERSE = tables()
SPLIT = [[2.0 * WEIGHTS[k] * float(DERIVATIVE[k, j]) for j in range(4)] for k in range(4)]


def roll(value, shift, axis):
    size = value.shape[axis]
    return pltpu.roll(value, shift % size, axis)


def local_node(shape, axis):
    return lax.broadcasted_iota(jnp.int32, shape, axis) % 4


def by_node(node, values):
    out = jnp.full(node.shape, values[3], jnp.float32)
    for k in range(3):
        out = jnp.where(node == k, jnp.float32(values[k]), out)
    return out


def primitives(parts):
    density = parts[0]
    inverse = 1.0 / density
    velocity = [parts[1 + d] * inverse for d in range(3)]
    square = velocity[0] * velocity[0] + velocity[1] * velocity[1] + velocity[2] * velocity[2]
    pressure = 0.4 * (parts[4] - 0.5 * density * square)
    return density, velocity, pressure, inverse


def sound_of(pressure, inverse):
    return jnp.sqrt(1.4 * pressure * inverse)


NAMES = ("r", "u", "v", "w", "p", "c", "s", "lr", "ls", "m1", "m2", "m3", "e")


def full_state(parts):
    density, velocity, pressure, inverse = primitives(parts)
    ratio = density / pressure
    return {
        "r": density,
        "u": velocity[0],
        "v": velocity[1],
        "w": velocity[2],
        "p": pressure,
        "c": sound_of(pressure, inverse),
        "s": ratio,
        "lr": jnp.log(density),
        "ls": jnp.log(ratio),
        "m1": parts[1],
        "m2": parts[2],
        "m3": parts[3],
        "e": parts[4],
    }


def mean_parts(a, b, log_a, log_b):
    total = a + b
    gap = a - b
    relative = gap / total
    square = relative * relative
    small = square < 0.01
    series = 1.0 + square * (1.0 / 3.0 + square * (1.0 / 5.0 + square * (1.0 / 7.0)))
    top = jnp.where(small, 0.5 * total, gap)
    bottom = jnp.where(small, series, log_a - log_b)
    return top, bottom


def pair_flux(a, b, normal):
    top, bottom = mean_parts(a["r"], b["r"], a["lr"], b["lr"])
    mass = top / bottom
    top, bottom = mean_parts(a["s"], b["s"], a["ls"], b["ls"])
    inverse_beta = bottom / top
    key = "uvw"[normal]
    flux0 = mass * (0.5 * (a[key] + b[key]))
    out = [flux0]
    for other in range(3):
        name = "uvw"[other]
        term = flux0 * (0.5 * (a[name] + b[name]))
        if other == normal:
            term = term + 0.5 * (a["p"] + b["p"])
        out.append(term)
    dot = 0.5 * (a["u"] * b["u"] + a["v"] * b["v"] + a["w"] * b["w"])
    out.append(
        flux0 * (dot + 2.5 * inverse_beta) + 0.5 * (a["p"] * b[key] + b["p"] * a[key])
    )
    return out


def dissipation(a, b, normal):
    key = "uvw"[normal]
    half = 0.5 * jnp.maximum(jnp.abs(a[key]) + a["c"], jnp.abs(b[key]) + b["c"])
    return [half * (b[q] - a[q]) for q in ("r", "m1", "m2", "m3", "e")]


def forward_kernel(in_ref, out_ref):
    row = jnp.max(in_ref[...], axis=0, keepdims=True)
    out_ref[...] = jnp.broadcast_to(row, out_ref.shape)


def transform(value, axis):
    node = local_node(value.shape, axis)
    total = None
    for offset in range(-3, 4):
        coefficients = [
            float(INVERSE[a, a + offset]) if 0 <= a + offset < 4 else 0.0 for a in range(4)
        ]
        shifted = value if offset == 0 else roll(value, -offset, axis)
        term = by_node(node, coefficients) * shifted
        total = term if total is None else total + term
    return total


def spread_sum(value, axis):
    index = lax.broadcasted_iota(jnp.int32, value.shape, axis)
    for step in (1, 2):
        other = jnp.where((index // step) % 2 == 1, roll(value, step, axis), roll(value, -step, axis))
        value = value + other
    return value


def raw_blending(layers):
    indicated = []
    for parts in layers:
        density, _, pressure, _ = primitives(parts)
        indicated.append(density * pressure)
    shape = indicated[0].shape
    node_y, node_z = local_node(shape, 0), local_node(shape, 1)
    degree = jnp.maximum(node_y, node_z)
    high = mid = low = None
    zero = jnp.zeros(shape, jnp.float32)
    for a in range(4):
        modes = sum(float(INVERSE[a, k]) * indicated[k] for k in range(4))
        modes = transform(transform(modes, 0), 1)
        square = modes * modes
        if a == 3:
            high = high + square
            continue
        top = jnp.where(degree == 3, square, zero)
        high = top if high is None else high + top
        if a == 2:
            mid = mid + jnp.where(degree < 3, square, zero)
            continue
        middle = jnp.where(degree == 2, square, zero)
        mid = middle if mid is None else mid + middle
        rest = jnp.where(degree < 2, square, zero)
        low = rest if low is None else low + rest
    high, mid, low = (spread_sum(spread_sum(v, 0), 1) for v in (high, mid, low))
    three = low + mid
    energy = jnp.maximum(high / (three + high + 1e-06), mid / (three + 1e-06))
    threshold = 0.5 * 10.0 ** (-1.8 * 4.0**0.25)
    sharpness = math.log(9999.0)
    raw = 1.0 / (1.0 + jnp.exp(-(sharpness / threshold) * (energy - threshold)))
    return jnp.minimum(raw, 0.5)


FIRST_X, MIDDLE_X = 5, 9
MIDDLE_Y = 9
OWN_Y = 9
X_TURN = 10


def x_slot(place, plane, own_ring):
    b_pair = place % 2 == 1
    if own_ring:
        if place == GX_SIZE - 1:
            return "Q"
        if place == 0:
            return "S"
        if place == X_TURN:
            return "R"
        return "P" if b_pair == (place < X_TURN) else "Q"
    if plane >= MIDDLE_X:
        return "Q" if b_pair else "R"
    return "P" if b_pair == (plane < FIRST_X) else "Q"


def y_slot(place, own_ring):
    b_pair, plane = place % 2 == 1, place // 2
    if own_ring:
        if plane < OWN_Y:
            if b_pair:
                return "R" if plane == OWN_Y - 1 else "P"
            return "Q"
        if plane >= MIDDLE_Y or (b_pair and plane == MIDDLE_Y - 1):
            return "R" if b_pair else "Q"
    if b_pair:
        return "Q"
    return "P" if plane < MIDDLE_Y else "R"


def sides():
    gx, gy = lax.axis_index("gx"), lax.axis_index("gy")
    core, plane, xl = gx & 1, gy >> 1, gy & 1
    first = plane < FIRST_X
    own_x = gy == 0
    turned = jnp.logical_or(gx == 0, gx > X_TURN)
    own_turned = jnp.logical_and(own_x, turned)
    own_straight = jnp.logical_and(own_x, jnp.logical_not(turned))
    middle = jnp.logical_and(plane >= FIRST_X, plane < MIDDLE_X)
    a_in_p = jnp.logical_or(middle, own_turned)
    a_in_q = jnp.logical_or(jnp.logical_and(first, jnp.logical_not(own_turned)), own_straight)
    own_y = gx == 0
    near = plane < OWN_Y
    b_in_p_y = jnp.logical_and(own_y, near)
    a_in_q_y = jnp.logical_and(own_y, jnp.logical_or(near, plane >= MIDDLE_Y))

    def side(a_pair, parity):
        return jnp.where(a_pair, 1 - parity, parity)

    along_x = [side(a_in_p, core), side(a_in_q, core), 1 - core]
    along_y = [
        side(jnp.logical_not(b_in_p_y), xl),
        side(a_in_q_y, xl),
        side(jnp.logical_not(own_y), xl),
    ]
    return along_x, along_y


def first_kernel(conserved_hbm, rows_hbm, raw_ref, xp, xq, xr, yp, yq, yr, held_ref, rows_ref, sems):
    copies = [
        pltpu.make_async_copy(conserved_hbm.at[:, x], held_ref.at[:, x], sems.at[x]) for x in range(4)
    ]
    for copy in copies:
        copy.start()
    best = None
    for x in range(4):
        copies[x].wait()
        _, velocity, pressure, inverse = primitives([held_ref[q, x] for q in range(5)])
        speed = (
            jnp.abs(velocity[0])
            + jnp.abs(velocity[1])
            + jnp.abs(velocity[2])
            + 3.0 * sound_of(pressure, inverse)
        )
        best = speed if best is None else jnp.maximum(best, speed)
    row = jnp.max(best, axis=0, keepdims=True)
    rows_ref[...] = jnp.broadcast_to(row[None], rows_ref.shape)
    sent = pltpu.make_async_copy(rows_ref, rows_hbm, sems.at[4])
    sent.start()
    raw = raw_blending([[held_ref[q, x] for q in range(5)] for x in range(4)])
    raw_ref[...] = raw

    def put_x(face_ref, x):
        for q in range(5):
            face_ref[q] = held_ref[q, x]
        face_ref[5] = raw

    def put_y(face_ref, row):
        for q in range(5):
            for x in range(4):
                face_ref[q, x : x + 1] = held_ref[q, x, row : row + 1]
        face_ref[5] = jnp.broadcast_to(raw[row : row + 1], (4, 128))

    def fill(side, put, face_ref, low, high):
        pl.when(side == 0)(lambda: put(face_ref, low))
        pl.when(side == 1)(lambda: put(face_ref, high))

    along_x, along_y = sides()
    for side, face_ref in zip(along_x, (xp, xq, xr), strict=True):
        fill(side, put_x, face_ref, 0, 3)
    for side, face_ref in zip(along_y, (yp, yq, yr), strict=True):
        fill(side, put_y, face_ref, 0, 15)
    sent.wait()


def physics_kernel(
    conserved_ref,
    raw_ref,
    xp,
    xq,
    xr,
    yp,
    yq,
    yr,
    xs,
    out_ref,
    blend_hbm,
    blend_ref,
    sem,
    state_ref,
    xprev_ref,
    xnext_ref,
    yprev_ref,
    ynext_ref,
):
    along_x, along_y = sides()
    for flags, refs, prev_ref, next_ref in (
        (along_x + along_x[2:], (xp, xq, xr, xs), xprev_ref, xnext_ref),
        (along_y, (yp, yq, yr), yprev_ref, ynext_ref),
    ):
        low = high = None
        for flag, ref in zip(flags, refs, strict=True):
            value = ref[...]
            up = flag.astype(jnp.float32)
            above, below = value * up, value * (1.0 - up)
            low = below if low is None else low + below
            high = above if high is None else high + above
        prev_ref[...] = low
        next_ref[...] = high

    raw = raw_ref[...]
    shape = raw.shape
    row = lax.broadcasted_iota(jnp.int32, shape, 0)
    node_y, node_z = row % 4, local_node(shape, 1)

    before = jnp.where(row < 4, jnp.broadcast_to(yprev_ref[5, 0:1], shape), roll(raw, 4, 0))
    after = jnp.where(row >= 12, jnp.broadcast_to(ynext_ref[5, 0:1], shape), roll(raw, -4, 0))
    around = jnp.maximum(xprev_ref[5], xnext_ref[5])
    around = jnp.maximum(around, jnp.maximum(before, after))
    around = jnp.maximum(around, jnp.maximum(roll(raw, 4, 1), roll(raw, -4, 1)))
    blend = jnp.maximum(raw, 0.5 * around)
    pick_z = (
        lax.broadcasted_iota(jnp.int32, (128, 32), 0) == 4 * lax.broadcasted_iota(jnp.int32, (128, 32), 1)
    ).astype(jnp.float32)
    compact = jnp.dot(
        blend, pick_z, precision=lax.Precision.HIGHEST, preferred_element_type=jnp.float32
    )
    for element in range(4):
        blend_ref[0, element : element + 1] = compact[4 * element : 4 * element + 1]
    sent = pltpu.make_async_copy(blend_ref, blend_hbm, sem)
    sent.start()
    keep = 1.0 - blend

    for x in range(4):
        state = full_state([conserved_ref[q, x] for q in range(5)])
        for i, name in enumerate(NAMES[:9]):
            state_ref[i, x] = state[name]

    def load(x):
        state = {name: state_ref[i, x] for i, name in enumerate(NAMES[:9])}
        for i, name in enumerate(NAMES[9:]):
            state[name] = conserved_ref[1 + i, x]
        return state

    def store(x, values, first=False):
        for q in range(5):
            out_ref[q, x] = values[q] if first else out_ref[q, x] + values[q]

    y_prev = full_state([yprev_ref[q] for q in range(5)])
    y_next = full_state([ynext_ref[q] for q in range(5)])
    edge = {}
    for i, name in enumerate(NAMES[:9]):
        edge[name] = jnp.concatenate([state_ref[i, x, 0:1] for x in range(4)], axis=0)
    for i, name in enumerate(NAMES[9:]):
        edge[name] = jnp.concatenate([conserved_ref[1 + i, x, 0:1] for x in range(4)], axis=0)
    low_face = [
        f - d for f, d in zip(pair_flux(y_prev, edge, 1), dissipation(y_prev, edge, 1), strict=True)
    ]

    def along(axis, node, x, state):
        normal = axis + 1
        one = jnp.ones(shape, jnp.float32)
        step = [SPLIT[0][1], SPLIT[1][2], SPLIT[2][3], 0.0]
        inner = node < 3
        weight_f = jnp.where(inner, keep * by_node(node, step) + blend, one)
        weight_d = jnp.where(inner, blend, one)
        weight_far = keep * by_node(node, [SPLIT[0][2], SPLIT[1][3], 0.0, SPLIT[3][0]])
        next_ = {}
        for name in NAMES:
            moved = roll(state[name], -1, axis)
            if axis == 0:
                moved = jnp.where(row == 15, jnp.broadcast_to(y_next[name][x : x + 1], shape), moved)
            next_[name] = moved
        flux = pair_flux(state, next_, normal)
        loss = dissipation(state, next_, normal)
        far = {
            name: jnp.where(node == 3, roll(state[name], 3, axis), roll(state[name], -2, axis))
            for name in ("r", "u", "v", "w", "p", "s", "lr", "ls")
        }
        cross = pair_flux(state, far, normal)
        inverse_weight = by_node(node, [-1.0 / w for w in WEIGHTS])
        out = []
        for q in range(5):
            near = weight_f * flux[q] - weight_d * loss[q]
            back = roll(near, 1, axis)
            if axis == 0:
                back = jnp.where(row == 0, jnp.broadcast_to(low_face[q][x : x + 1], shape), back)
            wide = weight_far * cross[q]
            taken = jnp.where(node >= 2, roll(wide, 2, axis), jnp.where(node == 0, roll(wide, -3, axis), 0.0))
            out.append(inverse_weight * (near - back + wide - taken))
        return out

    for x in range(4):
        state = load(x)
        in_y = along(0, node_y, x, state)
        in_z = along(1, node_z, x, state)
        store(x, [a + b for a, b in zip(in_y, in_z, strict=True)], first=True)

    def gather(other):
        return full_state([other[q] for q in range(5)])

    for first in range(4):
        for second in range(first + 1, 4):
            a, b = load(first), load(second)
            flux = pair_flux(a, b, 0)
            if second == first + 1:
                weight = keep * SPLIT[first][second] + blend
                loss = dissipation(a, b, 0)
                term = [weight * f - blend * d for f, d in zip(flux, loss, strict=True)]
            else:
                weight = keep * SPLIT[first][second]
                term = [weight * f for f in flux]
            store(first, [(-1.0 / WEIGHTS[first]) * t for t in term])
            store(second, [(1.0 / WEIGHTS[second]) * t for t in term])
    a, b = gather(xprev_ref), load(0)
    flux, loss = pair_flux(a, b, 0), dissipation(a, b, 0)
    store(0, [(1.0 / WEIGHTS[0]) * (f - d) for f, d in zip(flux, loss, strict=True)])
    a, b = load(3), gather(xnext_ref)
    flux, loss = pair_flux(a, b, 0), dissipation(a, b, 0)
    store(3, [(-1.0 / WEIGHTS[3]) * (f - d) for f, d in zip(flux, loss, strict=True)])
    sent.wait()


def scale_kernel(tendency_ref, speed_ref, out_ref):
    row = jnp.max(speed_ref[...], axis=0)
    top = jnp.max(row, axis=1, keepdims=True)
    step = 0.25 / top
    for q in range(5):
        for x in range(4):
            out_ref[q, x] = tendency_ref[q, x] * step


def call(kernel, outs, *args, scratch=(), **kwargs):
    return pl.pallas_call(
        kernel,
        out_shape=[jax.ShapeDtypeStruct(shape, jnp.float32) for shape in outs],
        scratch_shapes=list(scratch),
        compiler_params=pltpu.CompilerParams(vmem_limit_bytes=VMEM_BYTES),
        **kwargs,
    )(*args)


DEVICES = np.arange(math.prod(SIZES)).reshape(SIZES)
COUNT = DEVICES.size
GX_SIZE, GY_SIZE = math.prod(SIZES[:3]), math.prod(SIZES[3:])
Z_SIZE = SIZES[3]
Z_LEAD = 22
CHAIN_FACES = ("xP", "xQ", "xR", "yP", "yQ", "yR", "xS")


def trade(block, along_x, slot):
    grid = DEVICES.reshape(GX_SIZE, GY_SIZE)
    pairs = []
    if along_x:
        for place in range(GX_SIZE):
            for ring in range(GY_SIZE):
                if x_slot(place, ring // SIZES[4], ring == 0) == slot:
                    pairs.append((int(grid[place, ring]), int(grid[(place + 1) % GX_SIZE, ring])))
    else:
        for place in range(GY_SIZE):
            for ring in range(GX_SIZE):
                if y_slot(place, ring == 0) == slot:
                    pairs.append((int(grid[ring, place]), int(grid[ring, (place + 1) % GY_SIZE])))
    pairs += [(b, a) for a, b in pairs]
    return lax.ppermute(block, EVERY, pairs)


def z_groups():
    order = [Z_LEAD] + [z for z in range(Z_SIZE) if z != Z_LEAD]
    return DEVICES.transpose(0, 1, 2, 4, 3)[..., order].reshape(-1, Z_SIZE).tolist()


def plane_groups():
    index = DEVICES.transpose(3, 0, 1, 2, 4).reshape(Z_SIZE, -1)
    sizes = SIZES[:3] + SIZES[4:]
    lead = int(np.ravel_multi_index((sizes[0] - 1, sizes[1] // 2, 1, 0), sizes))
    order = [lead] + [i for i in range(index.shape[1]) if i != lead]
    return index[:, order].tolist()


def exchange(rows, groups):
    return lax.all_to_all(rows, EVERY, 0, 0, axis_index_groups=groups)


def body(conserved):
    plane = COUNT // Z_SIZE
    x_face, y_face = (6, 16, 128), (6, 4, 128)
    rows, raw, *faces = call(
        first_kernel,
        [(Z_SIZE, 1, 128), (16, 128)] + [x_face] * 3 + [y_face] * 3,
        pltpu.with_memory_space_constraint(conserved, pltpu.HBM),
        scratch=[
            pltpu.VMEM((5, 4, 16, 128), jnp.float32),
            pltpu.VMEM((Z_SIZE, 1, 128), jnp.float32),
            pltpu.SemaphoreType.DMA((5,)),
        ],
        in_specs=[pl.BlockSpec(memory_space=pltpu.HBM)],
        out_specs=[pl.BlockSpec(memory_space=pltpu.HBM)]
        + [pl.BlockSpec(memory_space=pltpu.VMEM)] * 7,
    )
    got = {}

    def swap(*names):
        for name in names:
            i = CHAIN_FACES.index("xR" if name == "xS" else name)
            got[name] = trade(faces[i], name[0] == "x", name[1])

    swap("xP", "yP")
    column = exchange(rows, z_groups())
    swap("xS", "xQ", "yQ", "xR")
    (forward,) = call(forward_kernel, [(plane, 1, 128)], column)
    speeds = exchange(forward, plane_groups())
    swap("yR")
    tendency, blending = call(
        physics_kernel,
        [(5, 4, 16, 128), (1, 4, 32)],
        conserved,
        raw,
        *(got[name] for name in CHAIN_FACES),
        out_specs=[pl.BlockSpec(memory_space=pltpu.VMEM), pl.BlockSpec(memory_space=pltpu.HBM)],
        scratch=[
            pltpu.VMEM((1, 4, 32), jnp.float32),
            pltpu.SemaphoreType.DMA,
            pltpu.VMEM((9, 4, 16, 128), jnp.float32),
            pltpu.VMEM(x_face, jnp.float32),
            pltpu.VMEM(x_face, jnp.float32),
            pltpu.VMEM(y_face, jnp.float32),
            pltpu.VMEM(y_face, jnp.float32),
        ],
    )
    (increment,) = call(scale_kernel, [(5, 4, 16, 128)], tendency, speeds)
    return increment, blending


def solution(mesh):
    split = Mesh(mesh.devices.reshape(GX_SIZE, GY_SIZE), EVERY)
    return jax.shard_map(
        body,
        mesh=split,
        in_specs=(P(None, "gx", "gy", None),),
        out_specs=(P(None, "gx", "gy", None), P("gx", "gy", None)),
        check_vma=False,
    )
```

```python
import math

import jax
import jax.numpy as jnp
import numpy as np
from jax import lax
from jax.experimental import pallas as pl
from jax.experimental.pallas import tpu as pltpu
from jax.sharding import Mesh
from jax.sharding import PartitionSpec as P


EVERY = ("gx", "gy")
SIZES = (2, 4, 2, 32, 2)

VMEM_BYTES = 6 << 20

WEIGHTS = (1.0 / 6.0, 5.0 / 6.0, 5.0 / 6.0, 1.0 / 6.0)


def tables():
    inverse_root = 1.0 / math.sqrt(5.0)
    points = np.array([-1.0, -inverse_root, inverse_root, 1.0])
    barycentric = np.array(
        [
            1.0 / np.prod([points[target] - points[other] for other in range(4) if other != target])
            for target in range(4)
        ]
    )
    derivative = np.zeros((4, 4))
    for target in range(4):
        for source in range(4):
            if target != source:
                derivative[target, source] = (
                    barycentric[source] / barycentric[target] / (points[target] - points[source])
                )
    legendre = np.stack(
        [np.ones(4), points, (3.0 * points**2 - 1.0) / 2.0, (5.0 * points**3 - 3.0 * points) / 2.0],
        1,
    )
    legendre = legendre * np.sqrt(np.arange(4) + 0.5)
    weight_column = np.array(WEIGHTS)[:, None]
    discrete_norms = np.sum(weight_column * legendre * legendre, 0)
    inverse = (weight_column * legendre).T / discrete_norms[:, None]
    return derivative, inverse


DERIVATIVE, INVERSE = tables()
SPLIT = [[2.0 * WEIGHTS[k] * float(DERIVATIVE[k, j]) for j in range(4)] for k in range(4)]


def roll(value, shift, axis):
    size = value.shape[axis]
    return pltpu.roll(value, shift % size, axis)


def local_node(shape, axis):
    return lax.broadcasted_iota(jnp.int32, shape, axis) % 4


def by_node(node, values):
    out = jnp.full(node.shape, values[3], jnp.float32)
    for k in range(3):
        out = jnp.where(node == k, jnp.float32(values[k]), out)
    return out


def primitives(parts):
    density = parts[0]
    inverse = 1.0 / density
    velocity = [parts[1 + d] * inverse for d in range(3)]
    square = velocity[0] * velocity[0] + velocity[1] * velocity[1] + velocity[2] * velocity[2]
    pressure = 0.4 * (parts[4] - 0.5 * density * square)
    return density, velocity, pressure, inverse


def sound_of(pressure, inverse):
    return jnp.sqrt(1.4 * pressure * inverse)


NAMES = ("r", "u", "v", "w", "p", "c", "s", "lr", "ls", "m1", "m2", "m3", "e")


def full_state(parts):
    density, velocity, pressure, inverse = primitives(parts)
    ratio = density / pressure
    return {
        "r": density,
        "u": velocity[0],
        "v": velocity[1],
        "w": velocity[2],
        "p": pressure,
        "c": sound_of(pressure, inverse),
        "s": ratio,
        "lr": jnp.log(density),
        "ls": jnp.log(ratio),
        "m1": parts[1],
        "m2": parts[2],
        "m3": parts[3],
        "e": parts[4],
    }


def mean_parts(a, b, log_a, log_b):
    total = a + b
    gap = a - b
    relative = gap / total
    square = relative * relative
    small = square < 0.01
    series = 1.0 + square * (1.0 / 3.0 + square * (1.0 / 5.0 + square * (1.0 / 7.0)))
    top = jnp.where(small, 0.5 * total, gap)
    bottom = jnp.where(small, series, log_a - log_b)
    return top, bottom


def pair_flux(a, b, normal):
    top, bottom = mean_parts(a["r"], b["r"], a["lr"], b["lr"])
    mass = top / bottom
    top, bottom = mean_parts(a["s"], b["s"], a["ls"], b["ls"])
    inverse_beta = bottom / top
    key = "uvw"[normal]
    flux0 = mass * (0.5 * (a[key] + b[key]))
    out = [flux0]
    for other in range(3):
        name = "uvw"[other]
        term = flux0 * (0.5 * (a[name] + b[name]))
        if other == normal:
            term = term + 0.5 * (a["p"] + b["p"])
        out.append(term)
    dot = 0.5 * (a["u"] * b["u"] + a["v"] * b["v"] + a["w"] * b["w"])
    out.append(
        flux0 * (dot + 2.5 * inverse_beta) + 0.5 * (a["p"] * b[key] + b["p"] * a[key])
    )
    return out


def dissipation(a, b, normal):
    key = "uvw"[normal]
    half = 0.5 * jnp.maximum(jnp.abs(a[key]) + a["c"], jnp.abs(b[key]) + b["c"])
    return [half * (b[q] - a[q]) for q in ("r", "m1", "m2", "m3", "e")]


def forward_kernel(in_ref, _, out_ref):
    row = jnp.max(in_ref[...], axis=0, keepdims=True)
    out_ref[...] = jnp.broadcast_to(row, out_ref.shape)


def transform(value, axis):
    node = local_node(value.shape, axis)
    total = None
    for offset in range(-3, 4):
        coefficients = [
            float(INVERSE[a, a + offset]) if 0 <= a + offset < 4 else 0.0 for a in range(4)
        ]
        shifted = value if offset == 0 else roll(value, -offset, axis)
        term = by_node(node, coefficients) * shifted
        total = term if total is None else total + term
    return total


def spread_sum(value, axis):
    index = lax.broadcasted_iota(jnp.int32, value.shape, axis)
    for step in (1, 2):
        other = jnp.where((index // step) % 2 == 1, roll(value, step, axis), roll(value, -step, axis))
        value = value + other
    return value


def raw_blending(layers):
    indicated = []
    for parts in layers:
        density, _, pressure, _ = primitives(parts)
        indicated.append(density * pressure)
    shape = indicated[0].shape
    node_y, node_z = local_node(shape, 0), local_node(shape, 1)
    degree = jnp.maximum(node_y, node_z)
    high = mid = low = None
    zero = jnp.zeros(shape, jnp.float32)
    for a in range(4):
        modes = sum(float(INVERSE[a, k]) * indicated[k] for k in range(4))
        modes = transform(transform(modes, 0), 1)
        square = modes * modes
        if a == 3:
            high = high + square
            continue
        top = jnp.where(degree == 3, square, zero)
        high = top if high is None else high + top
        if a == 2:
            mid = mid + jnp.where(degree < 3, square, zero)
            continue
        middle = jnp.where(degree == 2, square, zero)
        mid = middle if mid is None else mid + middle
        rest = jnp.where(degree < 2, square, zero)
        low = rest if low is None else low + rest
    high, mid, low = (spread_sum(spread_sum(v, 0), 1) for v in (high, mid, low))
    three = low + mid
    energy = jnp.maximum(high / (three + high + 1e-06), mid / (three + 1e-06))
    threshold = 0.5 * 10.0 ** (-1.8 * 4.0**0.25)
    sharpness = math.log(9999.0)
    raw = 1.0 / (1.0 + jnp.exp(-(sharpness / threshold) * (energy - threshold)))
    return jnp.minimum(raw, 0.5)


FIRST_X, MIDDLE_X = 5, 9
MIDDLE_Y = 9
OWN_Y = 9
X_TURN = 10


def x_slot(place, plane, own_ring):
    b_pair = place % 2 == 1
    if own_ring:
        if place == GX_SIZE - 1:
            return "Q"
        if place == 0:
            return "S"
        if place == X_TURN:
            return "R"
        return "P" if b_pair == (place < X_TURN) else "Q"
    if plane >= MIDDLE_X:
        return "Q" if b_pair else "R"
    return "P" if b_pair == (plane < FIRST_X) else "Q"


def y_slot(place, own_ring):
    b_pair, plane = place % 2 == 1, place // 2
    if own_ring:
        if plane < OWN_Y:
            if b_pair:
                return "R" if plane == OWN_Y - 1 else "P"
            return "Q"
        if plane >= MIDDLE_Y or (b_pair and plane == MIDDLE_Y - 1):
            return "R" if b_pair else "Q"
    if b_pair:
        return "Q"
    return "P" if plane < MIDDLE_Y else "R"


def sides():
    gx, gy = lax.axis_index("gx"), lax.axis_index("gy")
    core, plane, xl = gx & 1, gy >> 1, gy & 1
    first = plane < FIRST_X
    own_x = gy == 0
    turned = jnp.logical_or(gx == 0, gx > X_TURN)
    own_turned = jnp.logical_and(own_x, turned)
    own_straight = jnp.logical_and(own_x, jnp.logical_not(turned))
    middle = jnp.logical_and(plane >= FIRST_X, plane < MIDDLE_X)
    a_in_p = jnp.logical_or(middle, own_turned)
    a_in_q = jnp.logical_or(jnp.logical_and(first, jnp.logical_not(own_turned)), own_straight)
    own_y = gx == 0
    near = plane < OWN_Y
    b_in_p_y = jnp.logical_and(own_y, near)
    a_in_q_y = jnp.logical_and(own_y, jnp.logical_or(near, plane >= MIDDLE_Y))

    def side(a_pair, parity):
        return jnp.where(a_pair, 1 - parity, parity)

    along_x = [side(a_in_p, core), side(a_in_q, core), 1 - core]
    along_y = [
        side(jnp.logical_not(b_in_p_y), xl),
        side(a_in_q_y, xl),
        side(jnp.logical_not(own_y), xl),
    ]
    return along_x, along_y


def first_kernel(conserved_hbm, rows_hbm, raw_ref, xp, xq, xr, yp, yq, yr, held_ref, rows_ref, sems):
    copies = [
        pltpu.make_async_copy(conserved_hbm.at[:, x], held_ref.at[:, x], sems.at[x]) for x in range(4)
    ]
    for copy in copies:
        copy.start()
    best = None
    for x in range(4):
        copies[x].wait()
        _, velocity, pressure, inverse = primitives([held_ref[q, x] for q in range(5)])
        speed = (
            jnp.abs(velocity[0])
            + jnp.abs(velocity[1])
            + jnp.abs(velocity[2])
            + 3.0 * sound_of(pressure, inverse)
        )
        best = speed if best is None else jnp.maximum(best, speed)
    row = jnp.max(best, axis=0, keepdims=True)
    rows_ref[...] = jnp.broadcast_to(row[None], rows_ref.shape)
    sent = pltpu.make_async_copy(rows_ref, rows_hbm, sems.at[4])
    sent.start()
    raw = raw_blending([[held_ref[q, x] for q in range(5)] for x in range(4)])
    raw_ref[...] = raw

    def put_x(face_ref, x):
        for q in range(5):
            face_ref[q] = held_ref[q, x]
        face_ref[5] = raw

    def put_y(face_ref, row):
        for q in range(5):
            for x in range(4):
                face_ref[q, x : x + 1] = held_ref[q, x, row : row + 1]
        face_ref[5] = jnp.broadcast_to(raw[row : row + 1], (4, 128))

    def fill(side, put, face_ref, low, high):
        pl.when(side == 0)(lambda: put(face_ref, low))
        pl.when(side == 1)(lambda: put(face_ref, high))

    along_x, along_y = sides()
    for side, face_ref in zip(along_x, (xp, xq, xr), strict=True):
        fill(side, put_x, face_ref, 0, 3)
    for side, face_ref in zip(along_y, (yp, yq, yr), strict=True):
        fill(side, put_y, face_ref, 0, 15)
    sent.wait()


def is_ahead():
    gx, gy = lax.axis_index("gx"), lax.axis_index("gy")
    return jnp.logical_and(gy >> 1 < OWN_Y - 1, gx + gy > 0)


def ahead_kernel(conserved_ref, raw_ref, xp, xq, xr, xs, yp, yq, out_ref, blend_ref, *scratch):
    @pl.when(is_ahead())
    def _():
        physics(conserved_ref, raw_ref, (xp, xq, xr, xs), (yp, yq), out_ref, blend_ref, *scratch)


def rest_kernel(
    conserved_ref,
    raw_ref,
    xp,
    xq,
    xr,
    xs,
    yp,
    yq,
    yr,
    done_ref,
    smooth_ref,
    out_ref,
    blend_ref,
    *scratch,
):
    @pl.when(is_ahead())
    def _():
        out_ref[...] = done_ref[...]
        blend_ref[...] = smooth_ref[...]

    @pl.when(jnp.logical_not(is_ahead()))
    def _():
        physics(conserved_ref, raw_ref, (xp, xq, xr, xs), (yp, yq, yr), out_ref, blend_ref, *scratch)


def physics(
    conserved_ref,
    raw_ref,
    x_refs,
    y_refs,
    out_ref,
    blend_ref,
    state_ref,
    xprev_ref,
    xnext_ref,
    yprev_ref,
    ynext_ref,
):
    along_x, along_y = sides()
    for flags, refs, prev_ref, next_ref in (
        (along_x + along_x[2:], x_refs, xprev_ref, xnext_ref),
        (along_y[: len(y_refs)], y_refs, yprev_ref, ynext_ref),
    ):
        low = high = None
        for flag, ref in zip(flags, refs, strict=True):
            value = ref[...]
            up = flag.astype(jnp.float32)
            above, below = value * up, value * (1.0 - up)
            low = below if low is None else low + below
            high = above if high is None else high + above
        prev_ref[...] = low
        next_ref[...] = high

    raw = raw_ref[...]
    shape = raw.shape
    row = lax.broadcasted_iota(jnp.int32, shape, 0)
    node_y, node_z = row % 4, local_node(shape, 1)

    before = jnp.where(row < 4, jnp.broadcast_to(yprev_ref[5, 0:1], shape), roll(raw, 4, 0))
    after = jnp.where(row >= 12, jnp.broadcast_to(ynext_ref[5, 0:1], shape), roll(raw, -4, 0))
    around = jnp.maximum(xprev_ref[5], xnext_ref[5])
    around = jnp.maximum(around, jnp.maximum(before, after))
    around = jnp.maximum(around, jnp.maximum(roll(raw, 4, 1), roll(raw, -4, 1)))
    blend = jnp.maximum(raw, 0.5 * around)
    pick_z = (
        lax.broadcasted_iota(jnp.int32, (128, 32), 0) == 4 * lax.broadcasted_iota(jnp.int32, (128, 32), 1)
    ).astype(jnp.float32)
    compact = jnp.dot(
        blend, pick_z, precision=lax.Precision.HIGHEST, preferred_element_type=jnp.float32
    )
    for element in range(4):
        blend_ref[0, element : element + 1] = compact[4 * element : 4 * element + 1]
    keep = 1.0 - blend

    for x in range(4):
        state = full_state([conserved_ref[q, x] for q in range(5)])
        for i, name in enumerate(NAMES[:9]):
            state_ref[i, x] = state[name]

    def load(x):
        state = {name: state_ref[i, x] for i, name in enumerate(NAMES[:9])}
        for i, name in enumerate(NAMES[9:]):
            state[name] = conserved_ref[1 + i, x]
        return state

    def store(x, values, first=False):
        for q in range(5):
            out_ref[q, x] = values[q] if first else out_ref[q, x] + values[q]

    y_prev = full_state([yprev_ref[q] for q in range(5)])
    y_next = full_state([ynext_ref[q] for q in range(5)])
    edge = {}
    for i, name in enumerate(NAMES[:9]):
        edge[name] = jnp.concatenate([state_ref[i, x, 0:1] for x in range(4)], axis=0)
    for i, name in enumerate(NAMES[9:]):
        edge[name] = jnp.concatenate([conserved_ref[1 + i, x, 0:1] for x in range(4)], axis=0)
    low_face = [
        f - d for f, d in zip(pair_flux(y_prev, edge, 1), dissipation(y_prev, edge, 1), strict=True)
    ]

    def along(axis, node, x, state):
        normal = axis + 1
        one = jnp.ones(shape, jnp.float32)
        step = [SPLIT[0][1], SPLIT[1][2], SPLIT[2][3], 0.0]
        inner = node < 3
        weight_f = jnp.where(inner, keep * by_node(node, step) + blend, one)
        weight_d = jnp.where(inner, blend, one)
        weight_far = keep * by_node(node, [SPLIT[0][2], SPLIT[1][3], 0.0, SPLIT[3][0]])
        next_ = {}
        for name in NAMES:
            moved = roll(state[name], -1, axis)
            if axis == 0:
                moved = jnp.where(row == 15, jnp.broadcast_to(y_next[name][x : x + 1], shape), moved)
            next_[name] = moved
        flux = pair_flux(state, next_, normal)
        loss = dissipation(state, next_, normal)
        far = {
            name: jnp.where(node == 3, roll(state[name], 3, axis), roll(state[name], -2, axis))
            for name in ("r", "u", "v", "w", "p", "s", "lr", "ls")
        }
        cross = pair_flux(state, far, normal)
        inverse_weight = by_node(node, [-1.0 / w for w in WEIGHTS])
        out = []
        for q in range(5):
            near = weight_f * flux[q] - weight_d * loss[q]
            back = roll(near, 1, axis)
            if axis == 0:
                back = jnp.where(row == 0, jnp.broadcast_to(low_face[q][x : x + 1], shape), back)
            wide = weight_far * cross[q]
            taken = jnp.where(node >= 2, roll(wide, 2, axis), jnp.where(node == 0, roll(wide, -3, axis), 0.0))
            out.append(inverse_weight * (near - back + wide - taken))
        return out

    for x in range(4):
        state = load(x)
        in_y = along(0, node_y, x, state)
        in_z = along(1, node_z, x, state)
        store(x, [a + b for a, b in zip(in_y, in_z, strict=True)], first=True)

    def gather(other):
        return full_state([other[q] for q in range(5)])

    for first in range(4):
        for second in range(first + 1, 4):
            a, b = load(first), load(second)
            flux = pair_flux(a, b, 0)
            if second == first + 1:
                weight = keep * SPLIT[first][second] + blend
                loss = dissipation(a, b, 0)
                term = [weight * f - blend * d for f, d in zip(flux, loss, strict=True)]
            else:
                weight = keep * SPLIT[first][second]
                term = [weight * f for f in flux]
            store(first, [(-1.0 / WEIGHTS[first]) * t for t in term])
            store(second, [(1.0 / WEIGHTS[second]) * t for t in term])
    a, b = gather(xprev_ref), load(0)
    flux, loss = pair_flux(a, b, 0), dissipation(a, b, 0)
    store(0, [(1.0 / WEIGHTS[0]) * (f - d) for f, d in zip(flux, loss, strict=True)])
    a, b = load(3), gather(xnext_ref)
    flux, loss = pair_flux(a, b, 0), dissipation(a, b, 0)
    store(3, [(-1.0 / WEIGHTS[3]) * (f - d) for f, d in zip(flux, loss, strict=True)])


def scale_kernel(tendency_ref, smooth_ref, speed_ref, out_ref, blend_ref):
    blend_ref[...] = smooth_ref[...]
    row = jnp.max(speed_ref[...], axis=0)
    top = jnp.max(row, axis=1, keepdims=True)
    step = 0.25 / top
    for q in range(5):
        for x in range(4):
            out_ref[q, x] = tendency_ref[q, x] * step


def call(kernel, outs, *args, scratch=(), **kwargs):
    return pl.pallas_call(
        kernel,
        out_shape=[jax.ShapeDtypeStruct(shape, jnp.float32) for shape in outs],
        scratch_shapes=list(scratch),
        compiler_params=pltpu.CompilerParams(vmem_limit_bytes=VMEM_BYTES),
        **kwargs,
    )(*args)


DEVICES = np.arange(math.prod(SIZES)).reshape(SIZES)
COUNT = DEVICES.size
GX_SIZE, GY_SIZE = math.prod(SIZES[:3]), math.prod(SIZES[3:])
Z_SIZE = SIZES[3]
Z_LEAD = 22
CHAIN_FACES = ("xP", "xQ", "xR", "yP", "yQ", "yR", "xS")


def trade(block, along_x, slot):
    grid = DEVICES.reshape(GX_SIZE, GY_SIZE)
    pairs = []
    if along_x:
        for place in range(GX_SIZE):
            for ring in range(GY_SIZE):
                if x_slot(place, ring // SIZES[4], ring == 0) == slot:
                    pairs.append((int(grid[place, ring]), int(grid[(place + 1) % GX_SIZE, ring])))
    else:
        for place in range(GY_SIZE):
            for ring in range(GX_SIZE):
                if y_slot(place, ring == 0) == slot:
                    pairs.append((int(grid[ring, place]), int(grid[ring, (place + 1) % GY_SIZE])))
    pairs += [(b, a) for a, b in pairs]
    return lax.ppermute(block, EVERY, pairs)


def z_groups():
    order = [Z_LEAD] + [z for z in range(Z_SIZE) if z != Z_LEAD]
    return DEVICES.transpose(0, 1, 2, 4, 3)[..., order].reshape(-1, Z_SIZE).tolist()


def plane_groups():
    index = DEVICES.transpose(3, 0, 1, 2, 4).reshape(Z_SIZE, -1)
    sizes = SIZES[:3] + SIZES[4:]
    lead = int(np.ravel_multi_index((sizes[0] - 1, sizes[1] // 2, 1, 0), sizes))
    order = [lead] + [i for i in range(index.shape[1]) if i != lead]
    return index[:, order].tolist()


def exchange(rows, groups):
    return lax.all_to_all(rows, EVERY, 0, 0, axis_index_groups=groups)


def body(conserved):
    plane = COUNT // Z_SIZE
    x_face, y_face = (6, 16, 128), (6, 4, 128)
    rows, raw, *faces = call(
        first_kernel,
        [(Z_SIZE, 1, 128), (16, 128)] + [x_face] * 3 + [y_face] * 3,
        pltpu.with_memory_space_constraint(conserved, pltpu.HBM),
        scratch=[
            pltpu.VMEM((5, 4, 16, 128), jnp.float32),
            pltpu.VMEM((Z_SIZE, 1, 128), jnp.float32),
            pltpu.SemaphoreType.DMA((5,)),
        ],
        in_specs=[pl.BlockSpec(memory_space=pltpu.HBM)],
        out_specs=[pl.BlockSpec(memory_space=pltpu.HBM)]
        + [pl.BlockSpec(memory_space=pltpu.VMEM)] * 7,
    )
    got = {}

    def swap(*names):
        for name in names:
            i = CHAIN_FACES.index("xR" if name == "xS" else name)
            got[name] = trade(faces[i], name[0] == "x", name[1])

    swap("xP", "yP")
    column = exchange(rows, z_groups())
    swap("xS", "xQ", "yQ", "xR")
    scratch = [
        pltpu.VMEM((9, 4, 16, 128), jnp.float32),
        pltpu.VMEM(x_face, jnp.float32),
        pltpu.VMEM(x_face, jnp.float32),
        pltpu.VMEM(y_face, jnp.float32),
        pltpu.VMEM(y_face, jnp.float32),
    ]
    results = [(5, 4, 16, 128), (1, 4, 32)]
    early = [got[name] for name in ("xP", "xQ", "xR", "xS", "yP", "yQ")]
    ahead = call(ahead_kernel, results, conserved, raw, *early, scratch=scratch)
    (forward,) = call(forward_kernel, [(plane, 1, 128)], column, ahead[1])
    speeds = exchange(forward, plane_groups())
    swap("yR")
    rest = call(rest_kernel, results, conserved, raw, *early, got["yR"], *ahead, scratch=scratch)
    increment, blending = call(scale_kernel, results, *rest, speeds)
    return increment, blending


def solution(mesh):
    split = Mesh(mesh.devices.reshape(GX_SIZE, GY_SIZE), EVERY)
    return jax.shard_map(
        body,
        mesh=split,
        in_specs=(P(None, "gx", "gy", None),),
        out_specs=(P(None, "gx", "gy", None), P("gx", "gy", None)),
        check_vma=False,
    )
```

```python
import math

import jax
import jax.numpy as jnp
import numpy as np
from jax import lax
from jax.experimental import pallas as pl
from jax.experimental.pallas import tpu as pltpu
from jax.sharding import Mesh
from jax.sharding import PartitionSpec as P


EVERY = ("gx", "gy")
SIZES = (2, 4, 2, 32, 2)

VMEM_BYTES = 6 << 20

WEIGHTS = (1.0 / 6.0, 5.0 / 6.0, 5.0 / 6.0, 1.0 / 6.0)


def tables():
    inverse_root = 1.0 / math.sqrt(5.0)
    points = np.array([-1.0, -inverse_root, inverse_root, 1.0])
    barycentric = np.array(
        [
            1.0 / np.prod([points[target] - points[other] for other in range(4) if other != target])
            for target in range(4)
        ]
    )
    derivative = np.zeros((4, 4))
    for target in range(4):
        for source in range(4):
            if target != source:
                derivative[target, source] = (
                    barycentric[source] / barycentric[target] / (points[target] - points[source])
                )
    legendre = np.stack(
        [np.ones(4), points, (3.0 * points**2 - 1.0) / 2.0, (5.0 * points**3 - 3.0 * points) / 2.0],
        1,
    )
    legendre = legendre * np.sqrt(np.arange(4) + 0.5)
    weight_column = np.array(WEIGHTS)[:, None]
    discrete_norms = np.sum(weight_column * legendre * legendre, 0)
    inverse = (weight_column * legendre).T / discrete_norms[:, None]
    return derivative, inverse


DERIVATIVE, INVERSE = tables()
SPLIT = [[2.0 * WEIGHTS[k] * float(DERIVATIVE[k, j]) for j in range(4)] for k in range(4)]


def roll(value, shift, axis):
    size = value.shape[axis]
    return pltpu.roll(value, shift % size, axis)


def local_node(shape, axis):
    return lax.broadcasted_iota(jnp.int32, shape, axis) % 4


def by_node(node, values):
    out = jnp.full(node.shape, values[3], jnp.float32)
    for k in range(3):
        out = jnp.where(node == k, jnp.float32(values[k]), out)
    return out


def primitives(parts):
    density = parts[0]
    inverse = 1.0 / density
    velocity = [parts[1 + d] * inverse for d in range(3)]
    square = velocity[0] * velocity[0] + velocity[1] * velocity[1] + velocity[2] * velocity[2]
    pressure = 0.4 * (parts[4] - 0.5 * density * square)
    return density, velocity, pressure, inverse


def sound_of(pressure, inverse):
    return jnp.sqrt(1.4 * pressure * inverse)


NAMES = ("r", "u", "v", "w", "p", "c", "s", "lr", "ls", "m1", "m2", "m3", "e")


def full_state(parts):
    density, velocity, pressure, inverse = primitives(parts)
    ratio = density / pressure
    return {
        "r": density,
        "u": velocity[0],
        "v": velocity[1],
        "w": velocity[2],
        "p": pressure,
        "c": sound_of(pressure, inverse),
        "s": ratio,
        "lr": jnp.log(density),
        "ls": jnp.log(ratio),
        "m1": parts[1],
        "m2": parts[2],
        "m3": parts[3],
        "e": parts[4],
    }


def mean_parts(a, b, log_a, log_b):
    total = a + b
    gap = a - b
    relative = gap / total
    square = relative * relative
    small = square < 0.01
    series = 1.0 + square * (1.0 / 3.0 + square * (1.0 / 5.0 + square * (1.0 / 7.0)))
    top = jnp.where(small, 0.5 * total, gap)
    bottom = jnp.where(small, series, log_a - log_b)
    return top, bottom


def pair_flux(a, b, normal):
    top, bottom = mean_parts(a["r"], b["r"], a["lr"], b["lr"])
    mass = top / bottom
    top, bottom = mean_parts(a["s"], b["s"], a["ls"], b["ls"])
    inverse_beta = bottom / top
    key = "uvw"[normal]
    flux0 = mass * (0.5 * (a[key] + b[key]))
    out = [flux0]
    for other in range(3):
        name = "uvw"[other]
        term = flux0 * (0.5 * (a[name] + b[name]))
        if other == normal:
            term = term + 0.5 * (a["p"] + b["p"])
        out.append(term)
    dot = 0.5 * (a["u"] * b["u"] + a["v"] * b["v"] + a["w"] * b["w"])
    out.append(
        flux0 * (dot + 2.5 * inverse_beta) + 0.5 * (a["p"] * b[key] + b["p"] * a[key])
    )
    return out


def dissipation(a, b, normal):
    key = "uvw"[normal]
    half = 0.5 * jnp.maximum(jnp.abs(a[key]) + a["c"], jnp.abs(b[key]) + b["c"])
    return [half * (b[q] - a[q]) for q in ("r", "m1", "m2", "m3", "e")]


def forward_kernel(in_ref, out_ref):
    row = jnp.max(in_ref[...], axis=0, keepdims=True)
    out_ref[...] = jnp.broadcast_to(row, out_ref.shape)


def transform(value, axis):
    node = local_node(value.shape, axis)
    total = None
    for offset in range(-3, 4):
        coefficients = [
            float(INVERSE[a, a + offset]) if 0 <= a + offset < 4 else 0.0 for a in range(4)
        ]
        shifted = value if offset == 0 else roll(value, -offset, axis)
        term = by_node(node, coefficients) * shifted
        total = term if total is None else total + term
    return total


def spread_sum(value, axis):
    index = lax.broadcasted_iota(jnp.int32, value.shape, axis)
    for step in (1, 2):
        other = jnp.where((index // step) % 2 == 1, roll(value, step, axis), roll(value, -step, axis))
        value = value + other
    return value


def raw_blending(layers):
    indicated = []
    for parts in layers:
        density, _, pressure, _ = primitives(parts)
        indicated.append(density * pressure)
    shape = indicated[0].shape
    node_y, node_z = local_node(shape, 0), local_node(shape, 1)
    degree = jnp.maximum(node_y, node_z)
    high = mid = low = None
    zero = jnp.zeros(shape, jnp.float32)
    for a in range(4):
        modes = sum(float(INVERSE[a, k]) * indicated[k] for k in range(4))
        modes = transform(transform(modes, 0), 1)
        square = modes * modes
        if a == 3:
            high = high + square
            continue
        top = jnp.where(degree == 3, square, zero)
        high = top if high is None else high + top
        if a == 2:
            mid = mid + jnp.where(degree < 3, square, zero)
            continue
        middle = jnp.where(degree == 2, square, zero)
        mid = middle if mid is None else mid + middle
        rest = jnp.where(degree < 2, square, zero)
        low = rest if low is None else low + rest
    high, mid, low = (spread_sum(spread_sum(v, 0), 1) for v in (high, mid, low))
    three = low + mid
    energy = jnp.maximum(high / (three + high + 1e-06), mid / (three + 1e-06))
    threshold = 0.5 * 10.0 ** (-1.8 * 4.0**0.25)
    sharpness = math.log(9999.0)
    raw = 1.0 / (1.0 + jnp.exp(-(sharpness / threshold) * (energy - threshold)))
    return jnp.minimum(raw, 0.5)


FIRST_X, MIDDLE_X = 4, 9
MIDDLE_Y = 9
OWN_Y = 9
X_TURN = 10


def x_slot(place, plane, own_ring):
    b_pair = place % 2 == 1
    if own_ring:
        if place == GX_SIZE - 1:
            return "Q"
        if place == 0:
            return "S"
        if place == X_TURN:
            return "R"
        return "P" if b_pair == (place < X_TURN) else "Q"
    if plane >= MIDDLE_X:
        return "Q" if b_pair else "R"
    return "P" if b_pair == (plane < FIRST_X) else "Q"


def y_slot(place, own_ring):
    b_pair, plane = place % 2 == 1, place // 2
    if own_ring:
        if plane < OWN_Y:
            if b_pair:
                return "R" if plane == OWN_Y - 1 else "P"
            return "Q"
        if plane >= MIDDLE_Y or (b_pair and plane == MIDDLE_Y - 1):
            return "R" if b_pair else "Q"
    if b_pair:
        return "Q"
    return "P" if plane < MIDDLE_Y else "R"


def sides():
    gx, gy = lax.axis_index("gx"), lax.axis_index("gy")
    core, plane, xl = gx & 1, gy >> 1, gy & 1
    first = plane < FIRST_X
    own_x = gy == 0
    turned = jnp.logical_or(gx == 0, gx > X_TURN)
    own_turned = jnp.logical_and(own_x, turned)
    own_straight = jnp.logical_and(own_x, jnp.logical_not(turned))
    middle = jnp.logical_and(plane >= FIRST_X, plane < MIDDLE_X)
    a_in_p = jnp.logical_or(middle, own_turned)
    a_in_q = jnp.logical_or(jnp.logical_and(first, jnp.logical_not(own_turned)), own_straight)
    own_y = gx == 0
    near = plane < OWN_Y
    b_in_p_y = jnp.logical_and(own_y, near)
    a_in_q_y = jnp.logical_and(own_y, jnp.logical_or(near, plane >= MIDDLE_Y))

    def side(a_pair, parity):
        return jnp.where(a_pair, 1 - parity, parity)

    along_x = [side(a_in_p, core), side(a_in_q, core), 1 - core]
    along_y = [
        side(jnp.logical_not(b_in_p_y), xl),
        side(a_in_q_y, xl),
        side(jnp.logical_not(own_y), xl),
    ]
    return along_x, along_y


def first_kernel(conserved_hbm, rows_hbm, raw_ref, xp, xq, xr, yp, yq, yr, held_ref, rows_ref, sems):
    copies = [
        pltpu.make_async_copy(conserved_hbm.at[:, x], held_ref.at[:, x], sems.at[x]) for x in range(4)
    ]
    for copy in copies:
        copy.start()
    best = None
    for x in range(4):
        copies[x].wait()
        _, velocity, pressure, inverse = primitives([held_ref[q, x] for q in range(5)])
        speed = (
            jnp.abs(velocity[0])
            + jnp.abs(velocity[1])
            + jnp.abs(velocity[2])
            + 3.0 * sound_of(pressure, inverse)
        )
        best = speed if best is None else jnp.maximum(best, speed)
    row = jnp.max(best, axis=0, keepdims=True)
    rows_ref[...] = jnp.broadcast_to(row[None], rows_ref.shape)
    sent = pltpu.make_async_copy(rows_ref, rows_hbm, sems.at[4])
    sent.start()
    raw = raw_blending([[held_ref[q, x] for q in range(5)] for x in range(4)])
    raw_ref[...] = raw

    def put_x(face_ref, x):
        for q in range(5):
            face_ref[q] = held_ref[q, x]
        face_ref[5] = raw

    def put_y(face_ref, row):
        for q in range(5):
            for x in range(4):
                face_ref[q, x : x + 1] = held_ref[q, x, row : row + 1]
        face_ref[5] = jnp.broadcast_to(raw[row : row + 1], (4, 128))

    def fill(side, put, face_ref, low, high):
        pl.when(side == 0)(lambda: put(face_ref, low))
        pl.when(side == 1)(lambda: put(face_ref, high))

    along_x, along_y = sides()
    for side, face_ref in zip(along_x, (xp, xq, xr), strict=True):
        fill(side, put_x, face_ref, 0, 3)
    for side, face_ref in zip(along_y, (yp, yq, yr), strict=True):
        fill(side, put_y, face_ref, 0, 15)
    sent.wait()


def physics_kernel(
    conserved_ref,
    raw_ref,
    xp,
    xq,
    xr,
    yp,
    yq,
    yr,
    xs,
    out_ref,
    blend_ref,
    state_ref,
    xprev_ref,
    xnext_ref,
    yprev_ref,
    ynext_ref,
):
    along_x, along_y = sides()
    for flags, refs, prev_ref, next_ref in (
        (along_x + along_x[2:], (xp, xq, xr, xs), xprev_ref, xnext_ref),
        (along_y, (yp, yq, yr), yprev_ref, ynext_ref),
    ):
        low = high = None
        for flag, ref in zip(flags, refs, strict=True):
            value = ref[...]
            up = flag.astype(jnp.float32)
            above, below = value * up, value * (1.0 - up)
            low = below if low is None else low + below
            high = above if high is None else high + above
        prev_ref[...] = low
        next_ref[...] = high

    raw = raw_ref[...]
    shape = raw.shape
    row = lax.broadcasted_iota(jnp.int32, shape, 0)
    node_y, node_z = row % 4, local_node(shape, 1)

    before = jnp.where(row < 4, jnp.broadcast_to(yprev_ref[5, 0:1], shape), roll(raw, 4, 0))
    after = jnp.where(row >= 12, jnp.broadcast_to(ynext_ref[5, 0:1], shape), roll(raw, -4, 0))
    around = jnp.maximum(xprev_ref[5], xnext_ref[5])
    around = jnp.maximum(around, jnp.maximum(before, after))
    around = jnp.maximum(around, jnp.maximum(roll(raw, 4, 1), roll(raw, -4, 1)))
    blend = jnp.maximum(raw, 0.5 * around)
    pick_z = (
        lax.broadcasted_iota(jnp.int32, (128, 32), 0) == 4 * lax.broadcasted_iota(jnp.int32, (128, 32), 1)
    ).astype(jnp.float32)
    compact = jnp.dot(
        blend, pick_z, precision=lax.Precision.HIGHEST, preferred_element_type=jnp.float32
    )
    for element in range(4):
        blend_ref[0, element : element + 1] = compact[4 * element : 4 * element + 1]
    keep = 1.0 - blend

    for x in range(4):
        state = full_state([conserved_ref[q, x] for q in range(5)])
        for i, name in enumerate(NAMES[:9]):
            state_ref[i, x] = state[name]

    def load(x):
        state = {name: state_ref[i, x] for i, name in enumerate(NAMES[:9])}
        for i, name in enumerate(NAMES[9:]):
            state[name] = conserved_ref[1 + i, x]
        return state

    def store(x, values, first=False):
        for q in range(5):
            out_ref[q, x] = values[q] if first else out_ref[q, x] + values[q]

    y_prev = full_state([yprev_ref[q] for q in range(5)])
    y_next = full_state([ynext_ref[q] for q in range(5)])
    edge = {}
    for i, name in enumerate(NAMES[:9]):
        edge[name] = jnp.concatenate([state_ref[i, x, 0:1] for x in range(4)], axis=0)
    for i, name in enumerate(NAMES[9:]):
        edge[name] = jnp.concatenate([conserved_ref[1 + i, x, 0:1] for x in range(4)], axis=0)
    low_face = [
        f - d for f, d in zip(pair_flux(y_prev, edge, 1), dissipation(y_prev, edge, 1), strict=True)
    ]

    def along(axis, node, x, state):
        normal = axis + 1
        one = jnp.ones(shape, jnp.float32)
        step = [SPLIT[0][1], SPLIT[1][2], SPLIT[2][3], 0.0]
        inner = node < 3
        weight_f = jnp.where(inner, keep * by_node(node, step) + blend, one)
        weight_d = jnp.where(inner, blend, one)
        weight_far = keep * by_node(node, [SPLIT[0][2], SPLIT[1][3], 0.0, SPLIT[3][0]])
        next_ = {}
        for name in NAMES:
            moved = roll(state[name], -1, axis)
            if axis == 0:
                moved = jnp.where(row == 15, jnp.broadcast_to(y_next[name][x : x + 1], shape), moved)
            next_[name] = moved
        flux = pair_flux(state, next_, normal)
        loss = dissipation(state, next_, normal)
        far = {
            name: jnp.where(node == 3, roll(state[name], 3, axis), roll(state[name], -2, axis))
            for name in ("r", "u", "v", "w", "p", "s", "lr", "ls")
        }
        cross = pair_flux(state, far, normal)
        inverse_weight = by_node(node, [-1.0 / w for w in WEIGHTS])
        out = []
        for q in range(5):
            near = weight_f * flux[q] - weight_d * loss[q]
            back = roll(near, 1, axis)
            if axis == 0:
                back = jnp.where(row == 0, jnp.broadcast_to(low_face[q][x : x + 1], shape), back)
            wide = weight_far * cross[q]
            taken = jnp.where(node >= 2, roll(wide, 2, axis), jnp.where(node == 0, roll(wide, -3, axis), 0.0))
            out.append(inverse_weight * (near - back + wide - taken))
        return out

    for x in range(4):
        state = load(x)
        in_y = along(0, node_y, x, state)
        in_z = along(1, node_z, x, state)
        store(x, [a + b for a, b in zip(in_y, in_z, strict=True)], first=True)

    def gather(other):
        return full_state([other[q] for q in range(5)])

    for first in range(4):
        for second in range(first + 1, 4):
            a, b = load(first), load(second)
            flux = pair_flux(a, b, 0)
            if second == first + 1:
                weight = keep * SPLIT[first][second] + blend
                loss = dissipation(a, b, 0)
                term = [weight * f - blend * d for f, d in zip(flux, loss, strict=True)]
            else:
                weight = keep * SPLIT[first][second]
                term = [weight * f for f in flux]
            store(first, [(-1.0 / WEIGHTS[first]) * t for t in term])
            store(second, [(1.0 / WEIGHTS[second]) * t for t in term])
    a, b = gather(xprev_ref), load(0)
    flux, loss = pair_flux(a, b, 0), dissipation(a, b, 0)
    store(0, [(1.0 / WEIGHTS[0]) * (f - d) for f, d in zip(flux, loss, strict=True)])
    a, b = load(3), gather(xnext_ref)
    flux, loss = pair_flux(a, b, 0), dissipation(a, b, 0)
    store(3, [(-1.0 / WEIGHTS[3]) * (f - d) for f, d in zip(flux, loss, strict=True)])


def scale_kernel(tendency_ref, smooth_ref, speed_ref, out_ref, blend_ref):
    blend_ref[...] = smooth_ref[...]
    row = jnp.max(speed_ref[...], axis=0)
    top = jnp.max(row, axis=1, keepdims=True)
    step = 0.25 / top
    for q in range(5):
        for x in range(4):
            out_ref[q, x] = tendency_ref[q, x] * step


def call(kernel, outs, *args, scratch=(), **kwargs):
    return pl.pallas_call(
        kernel,
        out_shape=[jax.ShapeDtypeStruct(shape, jnp.float32) for shape in outs],
        scratch_shapes=list(scratch),
        compiler_params=pltpu.CompilerParams(vmem_limit_bytes=VMEM_BYTES),
        **kwargs,
    )(*args)


DEVICES = np.arange(math.prod(SIZES)).reshape(SIZES)
COUNT = DEVICES.size
GX_SIZE, GY_SIZE = math.prod(SIZES[:3]), math.prod(SIZES[3:])
Z_SIZE = SIZES[3]
Z_LEAD = 22
CHAIN_FACES = ("xP", "xQ", "xR", "yP", "yQ", "yR", "xS")


def trade(block, along_x, slot):
    grid = DEVICES.reshape(GX_SIZE, GY_SIZE)
    pairs = []
    if along_x:
        for place in range(GX_SIZE):
            for ring in range(GY_SIZE):
                if x_slot(place, ring // SIZES[4], ring == 0) == slot:
                    pairs.append((int(grid[place, ring]), int(grid[(place + 1) % GX_SIZE, ring])))
    else:
        for place in range(GY_SIZE):
            for ring in range(GX_SIZE):
                if y_slot(place, ring == 0) == slot:
                    pairs.append((int(grid[ring, place]), int(grid[ring, (place + 1) % GY_SIZE])))
    pairs += [(b, a) for a, b in pairs]
    return lax.ppermute(block, EVERY, pairs)


def z_groups():
    order = [Z_LEAD] + [z for z in range(Z_SIZE) if z != Z_LEAD]
    return DEVICES.transpose(0, 1, 2, 4, 3)[..., order].reshape(-1, Z_SIZE).tolist()


def plane_groups():
    index = DEVICES.transpose(3, 0, 1, 2, 4).reshape(Z_SIZE, -1)
    sizes = SIZES[:3] + SIZES[4:]
    lead = int(np.ravel_multi_index((sizes[0] - 1, sizes[1] // 2, 1, 0), sizes))
    order = [lead] + [i for i in range(index.shape[1]) if i != lead]
    return index[:, order].tolist()


def exchange(rows, groups):
    return lax.all_to_all(rows, EVERY, 0, 0, axis_index_groups=groups)


def body(conserved):
    plane = COUNT // Z_SIZE
    x_face, y_face = (6, 16, 128), (6, 4, 128)
    rows, raw, *faces = call(
        first_kernel,
        [(Z_SIZE, 1, 128), (16, 128)] + [x_face] * 3 + [y_face] * 3,
        pltpu.with_memory_space_constraint(conserved, pltpu.HBM),
        scratch=[
            pltpu.VMEM((5, 4, 16, 128), jnp.float32),
            pltpu.VMEM((Z_SIZE, 1, 128), jnp.float32),
            pltpu.SemaphoreType.DMA((5,)),
        ],
        in_specs=[pl.BlockSpec(memory_space=pltpu.HBM)],
        out_specs=[pl.BlockSpec(memory_space=pltpu.HBM)]
        + [pl.BlockSpec(memory_space=pltpu.VMEM)] * 7,
    )
    got = {}

    def swap(*names):
        for name in names:
            i = CHAIN_FACES.index("xR" if name == "xS" else name)
            got[name] = trade(faces[i], name[0] == "x", name[1])

    swap("xP", "yP")
    column = exchange(rows, z_groups())
    swap("xS", "xQ", "yQ", "xR")
    (forward,) = call(forward_kernel, [(plane, 1, 128)], column)
    speeds = exchange(forward, plane_groups())
    swap("yR")
    tendency, smooth = call(
        physics_kernel,
        [(5, 4, 16, 128), (1, 4, 32)],
        conserved,
        raw,
        *(got[name] for name in CHAIN_FACES),
        scratch=[
            pltpu.VMEM((9, 4, 16, 128), jnp.float32),
            pltpu.VMEM(x_face, jnp.float32),
            pltpu.VMEM(x_face, jnp.float32),
            pltpu.VMEM(y_face, jnp.float32),
            pltpu.VMEM(y_face, jnp.float32),
        ],
    )
    increment, blending = call(
        scale_kernel, [(5, 4, 16, 128), (1, 4, 32)], tendency, smooth, speeds
    )
    return increment, blending


def solution(mesh):
    split = Mesh(mesh.devices.reshape(GX_SIZE, GY_SIZE), EVERY)
    return jax.shard_map(
        body,
        mesh=split,
        in_specs=(P(None, "gx", "gy", None),),
        out_specs=(P(None, "gx", "gy", None), P("gx", "gy", None)),
        check_vma=False,
    )
```
